32 devices in a mesh: graph: 16 (over z, y, x), feat: 2 (over core).
Axes of the slice: x: 2, y: 2, z: 4, core: 2. Of those that a mesh axis runs over, the one named last changes fastest.
Arguments:
- features: bfloat16 [16384, 1024], P('graph', 'feat'), may hold values from -6 to 6
- rel_weight: bfloat16 [8, 1024, 1024], P(None, 'feat'), may hold values from -0.1875 to 0.1875
- self_weight: bfloat16 [1024, 1024], P('feat'), may hold values from -0.1875 to 0.1875
- type_bias: float32 [4, 1024], P(None, 'feat'), may hold values from -3 to 3
- node_type: int32 [16384], P('graph'), may hold values from 0 to 3
- tile_coef: bfloat16 [640, 128, 128], P('graph'), may hold values from -0.375 to 0.375
- tile_source: int32 [16, 40], P('graph'), may hold values from 0 to 23, as said below
- tile_target: int32 [16, 40], P('graph'), may hold values from 0 to 7
- tile_relation: int32 [16, 40], P('graph'), may hold values from 0 to 7
- send_block: int32 [16, 16], P('graph'), may hold values from 0 to 7
- send_live: int32 [16, 16], P('graph'), may hold values from 0 to 1, as said below
Outputs:
- updated: bfloat16 [16384, 1024], P('graph', 'feat')
The draws below stay inside these ranges and needn't reach their ends.
Inputs may be any that keep to these rules, and one draw needn't show every extreme that they name: send_live[s, s] is 0; partition q receives from 3 to 12 live blocks. `tile_source`: entries below 8 name the partition's own blocks; entry 8 + s names the block received from partition s and stands only where send_live[s, p] is 1; every live received block is named by some tile.
All inputs are finite; a program needn't handle non-finite values.
Results may differ from the reference program's by a relative error of at most 0.0065.
Values may be sent and summed in bfloat16 or wider, within the bound.
A program may use at most 64 MiB of HBM per device.

```python
import jax
import jax.numpy as jnp
from jax import lax

D = 1024
RELS = 8
NODE_TYPES = 4
BLOCK = 128
NODES_DEV = 1024
NODES = 16384
TILES_DEV = 40
N_GRAPH = 16


def boundary_plan(key):
    base = jax.random.fold_in(key, 7001)
    keys = jax.random.split(base, N_GRAPH)
    orders = jax.vmap(lambda k: jax.random.permutation(k, N_GRAPH))(keys)
    counts = jax.random.randint(jax.random.fold_in(key, 7002), (N_GRAPH,), N_GRAPH // 4, 3 * N_GRAPH // 4 + 1)
    ranks = jnp.argsort(orders, axis=1, stable=True)
    receivers = jnp.arange(N_GRAPH)[:, None]
    others = jnp.arange(N_GRAPH)[None, :]
    live_by_receiver = (ranks < counts[:, None]) & (others != receivers)
    return (orders, counts, live_by_receiver)


def draw_send_live(key, part):
    orders, counts, live_by_receiver = boundary_plan(key)
    return live_by_receiver.T.astype(jnp.int32)


def draw_tile_source(key, part):
    orders, counts, live_by_receiver = boundary_plan(key)
    count_blocks = NODES_DEV // BLOCK
    position = jnp.arange(TILES_DEV)[None, :]
    clamped = jnp.minimum(position, N_GRAPH - 1)
    sender = jnp.take_along_axis(orders, jnp.broadcast_to(clamped, (N_GRAPH, TILES_DEV)), axis=1)
    receivers = jnp.arange(N_GRAPH)[:, None]
    use_remote = (position < counts[:, None]) & (sender != receivers)
    local = jax.random.randint(jax.random.fold_in(key, 7003), (N_GRAPH, TILES_DEV), 0, count_blocks)
    return jnp.where(use_remote, count_blocks + sender, local).astype(jnp.int32)


def with_ends(values, own_key, low, high):
    index_at = [jax.random.randint(jax.random.fold_in(own_key, axis), (), 0, length) for axis, length in enumerate(values.shape)]
    widest = values.shape.index(max(values.shape))
    beside = index_at[:widest] + [(index_at[widest] + 1) % values.shape[widest]] + index_at[widest + 1:]
    return values.at[tuple(index_at)].set(low).at[tuple(beside)].set(high)


def level_of(rng, shape, pieces, smallest, largest):
    gain, own = 1.0, jax.random.fold_in(rng, 6)
    for dim, blocks in pieces:
        draws = jnp.exp(jax.random.uniform(jax.random.fold_in(own, dim), (blocks,), jnp.float32, smallest / len(pieces), largest / len(pieces)))
        gain = gain * jnp.repeat(draws, shape[dim] // blocks).reshape([-1 if axis == dim else 1 for axis in range(len(shape))])
    return gain


def scatter_about(stream_key, extent, width, bound, cuts=(), held_as=jnp.bfloat16):
    loudness = level_of(stream_key, extent, cuts, -0.22, 0.18) if cuts else 1.0
    entries = jax.random.normal(stream_key, extent, jnp.float32) * width * loudness
    return jnp.minimum(jnp.maximum(entries, -bound), bound).astype(held_as)


def setup_inputs(seed: int = 0) -> dict:
    arg_keys = jax.random.split(jax.random.key(seed), 12)
    features = scatter_about(arg_keys[0], (NODES, D), 1.0, 6.0, ((0, 16), (1, 2)))
    rel_weight = scatter_about(arg_keys[1], (RELS, D, D), D ** -0.5, 0.1875, ((1, 2),))
    self_weight = scatter_about(arg_keys[2], (D, D), D ** -0.5, 0.1875, ((0, 2),))
    type_bias = scatter_about(arg_keys[3], (NODE_TYPES, D), 0.5, 3.0, ((1, 2),), jnp.float32)
    node_type = with_ends(jax.random.randint(arg_keys[4], (NODES,), 0, NODE_TYPES), jax.random.fold_in(arg_keys[4], 1), 0, NODE_TYPES - 1).astype(jnp.int32)
    tile_coef = scatter_about(arg_keys[5], (N_GRAPH * TILES_DEV, BLOCK, BLOCK), (2 * BLOCK) ** -0.5, 0.375, ((0, 16),))
    tile_source = draw_tile_source(jax.random.fold_in(arg_keys[11], 71), 0)
    tile_target = with_ends(jax.random.randint(arg_keys[7], (N_GRAPH, TILES_DEV), 0, NODES_DEV // BLOCK), jax.random.fold_in(arg_keys[7], 1), 0, (NODES_DEV // BLOCK) - 1).astype(jnp.int32)
    tile_relation = with_ends(jax.random.randint(arg_keys[8], (N_GRAPH, TILES_DEV), 0, RELS), jax.random.fold_in(arg_keys[8], 1), 0, RELS - 1).astype(jnp.int32)
    send_block = with_ends(jax.random.randint(arg_keys[9], (N_GRAPH, N_GRAPH), 0, NODES_DEV // BLOCK), jax.random.fold_in(arg_keys[9], 1), 0, (NODES_DEV // BLOCK) - 1).astype(jnp.int32)
    send_live = draw_send_live(jax.random.fold_in(arg_keys[11], 71), 0)
    return {"features": features, "rel_weight": rel_weight, "self_weight": self_weight, "type_bias": type_bias, "node_type": node_type, "tile_coef": tile_coef, "tile_source": tile_source, "tile_target": tile_target, "tile_relation": tile_relation, "send_block": send_block, "send_live": send_live}


def reference(features, rel_weight, self_weight, type_bias, node_type, tile_coef, tile_source, tile_target, tile_relation, send_block, send_live):
    count_blocks = NODES_DEV // BLOCK
    blocked = features.reshape(N_GRAPH, count_blocks, BLOCK, D)
    coef_all = tile_coef.reshape(N_GRAPH, TILES_DEV, BLOCK, BLOCK)
    senders = jnp.arange(N_GRAPH, dtype=jnp.int32)
    kinds = jnp.arange(NODE_TYPES, dtype=jnp.int32)
    slots = jnp.arange(RELS * count_blocks, dtype=jnp.int32)

    def one_part(part):
        local = blocked[part]
        picks = send_block[:, part].astype(jnp.int32)
        remote = blocked[senders, picks] * send_live[:, part].astype(features.dtype)[:, None, None]
        table = jnp.concatenate([local, remote], axis=0)
        sources = table[tile_source[part].astype(jnp.int32)]
        products = jnp.einsum("tij,tjd->tid", coef_all[part].astype(jnp.float32), sources.astype(jnp.float32), precision=lax.Precision.HIGHEST)
        slot = tile_relation[part] * count_blocks + tile_target[part]
        onehot = (slot[:, None] == slots[None, :]).astype(jnp.float32)
        summed = jnp.einsum("tk,tbd->kbd", onehot, products, precision=lax.Precision.HIGHEST)
        aggregate = summed.reshape(RELS, NODES_DEV, D).astype(jnp.bfloat16)
        rows = local.reshape(NODES_DEV, D)
        partial_value = jnp.dot(rows, self_weight, preferred_element_type=jnp.float32)
        for relation in range(RELS):
            partial_value = partial_value + jnp.dot(aggregate[relation], rel_weight[relation], preferred_element_type=jnp.float32)
        types = lax.dynamic_slice(node_type, (part * NODES_DEV,), (NODES_DEV,))
        type_onehot = (types[:, None] == kinds[None, :]).astype(jnp.float32)
        biased = partial_value + jnp.dot(type_onehot, type_bias, precision=lax.Precision.HIGHEST)
        return jnp.maximum(biased, 0.0).astype(jnp.bfloat16)

    updated = lax.map(one_part, jnp.arange(N_GRAPH, dtype=jnp.int32))
    return updated.reshape(NODES, D)
```

```python
import functools

import jax
import jax.numpy as jnp
from jax import lax
from jax.experimental import pallas as pl
from jax.experimental.pallas import tpu as pltpu
from jax.sharding import PartitionSpec as P

MESH = pl.DeviceIdType.MESH


def partner(me, step, count):
    other, bit = 0, 1
    while bit < count:
        other = other + ((me // bit + step // bit) % 2) * bit
        bit *= 2
    return other


def exchange_kernel(
    groups,
    shards,
    block,
    send_block,
    send_live,
    x_ref,
    x_blocks,
    rel_ref,
    self_ref,
    bias_ref,
    type_ref,
    received,
    w_out,
    h_out,
    s_out,
    outgoing,
    x_far,
    w_all,
    h_vmem,
    s_vmem,
    send_sem,
    recv_sem,
    pass_send,
    pass_recv,
    side_send,
    side_recv,
    local_sem,
    h_sem,
):
    me, mine = lax.axis_index("graph"), lax.axis_index("feat")
    rows, width = x_ref.shape
    relations = rel_ref.shape[0]

    def columns(shard):
        return pl.ds(pl.multiple_of(shard * width, width), width)

    own_rel = pltpu.make_async_copy(
        rel_ref.at[:, :, columns(mine)], w_all.at[mine, pl.ds(0, relations)], local_sem.at[0]
    )
    own_self = pltpu.make_async_copy(
        self_ref.at[:, columns(mine)], w_all.at[mine, relations], local_sem.at[1]
    )
    own_rel.start()
    own_self.start()

    def gather(q, carry):
        picked = x_blocks[send_block[0, q]].astype(jnp.float32)
        outgoing[q] = (picked * send_live[0, q].astype(jnp.float32)).astype(outgoing.dtype)
        return carry

    lax.fori_loop(0, groups, gather, 0)

    barrier = pltpu.get_barrier_semaphore()

    def greet(step, carry):
        pl.semaphore_signal(
            barrier, inc=1, device_id=(partner(me, step, groups), mine), device_id_type=MESH
        )
        return carry

    lax.fori_loop(1, groups, greet, 0)
    for e in range(1, shards):
        pl.semaphore_signal(
            barrier, inc=1, device_id=(me, (mine + e) % shards), device_id_type=MESH
        )
    pl.semaphore_wait(barrier, groups - 1 + shards - 1)

    def boundary(step):
        other = partner(me, step, groups)
        return pltpu.make_async_remote_copy(
            src_ref=outgoing.at[other],
            dst_ref=received.at[mine, me],
            send_sem=send_sem.at[step],
            recv_sem=recv_sem.at[step],
            device_id=(other, mine),
            device_id_type=MESH,
        )

    def send(i, carry):
        boundary(groups - 1 - i).start()
        return carry

    lax.fori_loop(0, groups - 1, send, 0)

    def side(e):
        peer = (mine + e) % shards
        pairs = (
            (x_ref, x_far.at[mine]),
            (self_ref.at[:, columns(peer)], w_all.at[mine, relations]),
            (rel_ref.at[:, :, columns(peer)], w_all.at[mine, pl.ds(0, relations)]),
        )
        return [
            pltpu.make_async_remote_copy(
                src_ref=src,
                dst_ref=dst,
                send_sem=side_send.at[e - 1, i],
                recv_sem=side_recv.at[e - 1, i],
                device_id=(me, peer),
                device_id_type=MESH,
            )
            for i, (src, dst) in enumerate(pairs)
        ]

    sides = [copy for e in range(1, shards) for copy in side(e)]
    for copy in sides:
        copy.start()
    own_rel.wait()
    own_self.wait()
    for copy in sides:
        copy.wait()
    w_copy = pltpu.make_async_copy(
        w_all.at[:, pl.ds(0, relations)], w_out, local_sem.at[2]
    )
    w_copy.start()

    chunk = 2 * block

    def full_dot(start, relation):
        rows_at = pl.ds(start, chunk)
        total = jnp.dot(
            x_ref[rows_at, :], w_all[mine, relation], preferred_element_type=jnp.float32
        )
        for e in range(1, shards):
            peer = (mine + e) % shards
            total = total + jnp.dot(
                x_far[peer, rows_at, :], w_all[peer, relation], preferred_element_type=jnp.float32
            )
        return total

    def transform(relation, carry):
        def part(i, inner):
            start = pl.multiple_of(i * chunk, chunk)
            h_vmem[relation, pl.ds(start, chunk), :] = full_dot(start, relation).astype(h_vmem.dtype)
            return inner

        return lax.fori_loop(0, rows // chunk, part, carry)

    lax.fori_loop(0, relations, transform, 0)

    def own_part(i, carry):
        start = pl.multiple_of(i * chunk, chunk)
        s_vmem[pl.ds(start, chunk), :] = full_dot(start, relations)
        return carry

    lax.fori_loop(0, rows // chunk, own_part, 0)
    lanes = type_ref.shape[1]
    for i in range(rows // lanes):
        kinds = jnp.transpose(jnp.broadcast_to(type_ref[i : i + 1, :], (lanes, lanes)))
        kinds = jnp.concatenate([kinds] * (width // lanes), axis=1)
        total = s_vmem[i * lanes : (i + 1) * lanes, :]
        for kind in range(bias_ref.shape[0]):
            total = total + jnp.where(kinds == kind, bias_ref[kind : kind + 1, :], 0.0)
        s_vmem[i * lanes : (i + 1) * lanes, :] = total

    h_copy = pltpu.make_async_copy(h_vmem, h_out, h_sem.at[0])
    s_copy = pltpu.make_async_copy(s_vmem, s_out, h_sem.at[1])

    def forward(step, e):
        other = partner(me, step, groups)
        return pltpu.make_async_remote_copy(
            src_ref=received.at[mine, other],
            dst_ref=received.at[mine, other],
            send_sem=pass_send.at[e - 1, step],
            recv_sem=pass_recv.at[e - 1, step],
            device_id=(me, (mine + e) % shards),
            device_id_type=MESH,
        )

    def arrived(i, carry):
        step = groups - 1 - i
        boundary(step).wait_recv()
        for e in range(1, shards):
            forward(step, e).start()
        return carry

    h_copy.start()
    s_copy.start()
    lax.fori_loop(0, groups - 1, arrived, 0)

    def finish(i, carry):
        step = groups - 1 - i
        boundary(step).wait_send()
        for e in range(1, shards):
            forward(step, e).wait_send()
            origin = (mine + shards - e) % shards
            other = partner(me, step, groups)
            pltpu.make_async_remote_copy(
                src_ref=received.at[origin, other],
                dst_ref=received.at[origin, other],
                send_sem=pass_send.at[e - 1, step],
                recv_sem=pass_recv.at[e - 1, step],
                device_id=(me, (mine + e) % shards),
                device_id_type=MESH,
            ).wait_recv()
        return carry

    lax.fori_loop(0, groups - 1, finish, 0)
    w_copy.wait()
    h_copy.wait()
    s_copy.wait()


def tile_kernel(
    tile_source,
    tile_target,
    tile_relation,
    coef_hbm,
    h_hbm,
    s_hbm,
    received,
    w_hbm,
    out_ref,
    coef,
    h_tiles,
    x_tiles,
    w_vmem,
    total,
    tile_sem,
    w_sem,
    base_sem,
):
    tiles, block, _ = coef.shape
    shards = w_vmem.shape[1]
    own = total.shape[0] // block

    def rows_of(index):
        return pl.ds(pl.multiple_of(index * block, block), block)

    def local_copy(t):
        return pltpu.make_async_copy(
            h_hbm.at[tile_relation[0, t], rows_of(tile_source[0, t])], h_tiles.at[t], tile_sem.at[t]
        )

    def remote_copy(t):
        return pltpu.make_async_copy(
            received.at[:, tile_source[0, t] - own], x_tiles.at[t], tile_sem.at[t]
        )

    coef_copy = pltpu.make_async_copy(coef_hbm, coef, base_sem.at[0])
    total_copy = pltpu.make_async_copy(s_hbm, total, base_sem.at[1])
    coef_copy.start()
    total_copy.start()

    def start(t, carry):
        @pl.when(tile_source[0, t] < own)
        def _():
            local_copy(t).start()

        @pl.when(tile_source[0, t] >= own)
        def _():
            remote_copy(t).start()

        return carry

    lax.fori_loop(0, tiles, start, 0)
    w_copies = [
        pltpu.make_async_copy(w_hbm.at[:, r], w_vmem.at[r], w_sem.at[r])
        for r in range(w_vmem.shape[0])
    ]
    for copy in w_copies:
        copy.start()
    coef_copy.wait()
    total_copy.wait()

    def add(t, source):
        at = rows_of(tile_target[0, t])
        total[at, :] += jnp.dot(coef[t], source, preferred_element_type=jnp.float32)

    def local(t, carry):
        @pl.when(tile_source[0, t] < own)
        def _():
            local_copy(t).wait()
            add(t, h_tiles[t])

        return carry

    lax.fori_loop(0, tiles, local, 0)
    for copy in w_copies:
        copy.wait()

    def remote(t, carry):
        @pl.when(tile_source[0, t] >= own)
        def _():
            remote_copy(t).wait()
            relation = tile_relation[0, t]
            moved = jnp.dot(x_tiles[t, 0], w_vmem[relation, 0], preferred_element_type=jnp.float32)
            for e in range(1, shards):
                moved = moved + jnp.dot(
                    x_tiles[t, e], w_vmem[relation, e], preferred_element_type=jnp.float32
                )
            add(t, moved.astype(coef.dtype))

        return carry

    lax.fori_loop(0, tiles, remote, 0)
    out_ref[...] = jnp.maximum(total[...], 0.0).astype(out_ref.dtype)


def per_device(
    groups,
    shards,
    features,
    rel_weight,
    self_weight,
    type_bias,
    node_type,
    tile_coef,
    tile_source,
    tile_target,
    tile_relation,
    send_block,
    send_live,
):
    rows, width = features.shape
    tiles, block, _ = tile_coef.shape
    relations = rel_weight.shape[0]
    kind = features.dtype
    smem = pl.BlockSpec(memory_space=pltpu.SMEM)
    vmem = pl.BlockSpec(memory_space=pltpu.VMEM)
    anywhere = pl.BlockSpec(memory_space=pl.ANY)
    dma = pltpu.SemaphoreType.DMA
    received, weights, moved, base = pl.pallas_call(
        functools.partial(exchange_kernel, groups, shards, block),
        out_shape=(
            jax.ShapeDtypeStruct((shards, groups, block, width), kind),
            jax.ShapeDtypeStruct((shards, relations, width, width), kind),
            jax.ShapeDtypeStruct((relations, rows, width), kind),
            jax.ShapeDtypeStruct((rows, width), jnp.float32),
        ),
        in_specs=[smem, smem, vmem, vmem, anywhere, anywhere, vmem, vmem],
        out_specs=(anywhere,) * 4,
        scratch_shapes=[
            pltpu.VMEM((groups, block, width), kind),
            pltpu.VMEM((shards, rows, width), kind),
            pltpu.VMEM((shards, relations + 1, width, width), kind),
            pltpu.VMEM((relations, rows, width), kind),
            pltpu.VMEM((rows, width), jnp.float32),
            dma((groups,)),
            dma((groups,)),
            dma((max(shards - 1, 1), groups)),
            dma((max(shards - 1, 1), groups)),
            dma((max(shards - 1, 1), 3)),
            dma((max(shards - 1, 1), 3)),
            dma((3,)),
            dma((2,)),
        ],
        compiler_params=pltpu.CompilerParams(
            collective_id=0, has_side_effects=True, vmem_limit_bytes=48 * 2**20
        ),
        name="exchange",
    )(
        send_block,
        send_live,
        features,
        features.reshape(rows // block, block, width),
        rel_weight,
        self_weight,
        type_bias,
        node_type.reshape(rows // block, block),
    )
    return pl.pallas_call(
        tile_kernel,
        out_shape=jax.ShapeDtypeStruct((rows, width), kind),
        in_specs=[smem] * 3 + [anywhere] * 5,
        out_specs=vmem,
        scratch_shapes=[
            pltpu.VMEM((tiles, block, block), kind),
            pltpu.VMEM((tiles, block, width), kind),
            pltpu.VMEM((tiles, shards, block, width), kind),
            pltpu.VMEM((relations, shards, width, width), kind),
            pltpu.VMEM((rows, width), jnp.float32),
            dma((tiles,)),
            dma((relations,)),
            dma((2,)),
        ],
        compiler_params=pltpu.CompilerParams(vmem_limit_bytes=56 * 2**20),
        name="tiles",
    )(tile_source, tile_target, tile_relation, tile_coef, moved, base, received, weights)


def solution(mesh):
    placed = (
        P("graph", "feat"),
        P(None, "feat", None),
        P("feat", None),
        P(None, "feat"),
        P("graph"),
        P("graph", None, None),
        P("graph", None),
        P("graph", None),
        P("graph", None),
        P("graph", None),
        P("graph", None),
    )
    groups, shards = mesh.shape["graph"], mesh.shape["feat"]
    return jax.shard_map(
        functools.partial(per_device, groups, shards),
        mesh=mesh,
        in_specs=placed,
        out_specs=P("graph", "feat"),
        check_vma=False,
    )
```

```python
import functools

import jax
import jax.numpy as jnp
from jax import lax
from jax.experimental import pallas as pl
from jax.experimental.pallas import tpu as pltpu
from jax.sharding import PartitionSpec as P

MESH = pl.DeviceIdType.MESH
VMEM = 67_043_328


def partner(me, step, count):
    other, bit = 0, 1
    while bit < count:
        other = other + ((me // bit + step // bit) % 2) * bit
        bit *= 2
    return other


def exchange_kernel(
    groups,
    shards,
    block,
    send_block,
    send_live,
    tile_source,
    tile_target,
    tile_relation,
    bias_ref,
    type_ref,
    x_hbm,
    rel_ref,
    self_ref,
    coef_hbm,
    received,
    w_out,
    s_out,
    outgoing,
    x_own,
    x_far,
    w_all,
    h_vmem,
    s_vmem,
    coef,
    products,
    send_sem,
    recv_sem,
    pass_send,
    pass_recv,
    side_send,
    side_recv,
    local_sem,
):
    me, mine = lax.axis_index("graph"), lax.axis_index("feat")
    blocks, _, width = x_own.shape
    relations = rel_ref.shape[0]
    tiles = coef.shape[0]

    def columns(shard):
        return pl.ds(pl.multiple_of(shard * width, width), width)

    barrier = pltpu.get_barrier_semaphore()

    def greet(step, carry):
        pl.semaphore_signal(
            barrier, inc=1, device_id=(partner(me, step, groups), mine), device_id_type=MESH
        )
        return carry

    lax.fori_loop(1, groups, greet, 0)
    for e in range(1, shards):
        pl.semaphore_signal(
            barrier, inc=1, device_id=(me, (mine + e) % shards), device_id_type=MESH
        )

    x_copy = pltpu.make_async_copy(x_hbm, x_own, local_sem.at[3])
    own_rel = pltpu.make_async_copy(
        rel_ref.at[:, :, columns(mine)], w_all.at[mine, pl.ds(0, relations)], local_sem.at[0]
    )
    own_self = pltpu.make_async_copy(
        self_ref.at[:, columns(mine)], w_all.at[mine, relations], local_sem.at[1]
    )
    coef_copy = pltpu.make_async_copy(coef_hbm, coef, local_sem.at[4])
    x_copy.start()
    own_rel.start()
    own_self.start()
    coef_copy.start()
    x_copy.wait()

    def gather(q, carry):
        picked = x_own[send_block[0, q]].astype(jnp.float32)
        outgoing[q] = (picked * send_live[0, q].astype(jnp.float32)).astype(outgoing.dtype)
        return carry

    lax.fori_loop(0, groups, gather, 0)
    pl.semaphore_wait(barrier, groups - 1 + shards - 1)

    def boundary(step):
        other = partner(me, step, groups)
        return pltpu.make_async_remote_copy(
            src_ref=outgoing.at[other],
            dst_ref=received.at[mine, me],
            send_sem=send_sem.at[step],
            recv_sem=recv_sem.at[step],
            device_id=(other, mine),
            device_id_type=MESH,
        )

    def send(step, carry):
        boundary(step).start()
        return carry

    lax.fori_loop(1, groups, send, 0)

    def side(e):
        peer = (mine + e) % shards
        pairs = (
            (x_own, x_far.at[mine]),
            (self_ref.at[:, columns(peer)], w_all.at[mine, relations]),
            (rel_ref.at[:, :, columns(peer)], w_all.at[mine, pl.ds(0, relations)]),
        )
        return [
            pltpu.make_async_remote_copy(
                src_ref=src,
                dst_ref=dst,
                send_sem=side_send.at[e - 1, i],
                recv_sem=side_recv.at[e - 1, i],
                device_id=(me, peer),
                device_id_type=MESH,
            )
            for i, (src, dst) in enumerate(pairs)
        ]

    sides = [copy for e in range(1, shards) for copy in side(e)]
    for copy in sides:
        copy.start()
    own_rel.wait()
    own_self.wait()
    for copy in sides:
        copy.wait()
    w_copy = pltpu.make_async_copy(
        w_all.at[:, pl.ds(0, relations)], w_out, local_sem.at[2]
    )
    w_copy.start()

    chunk = 2

    def full_dot(start, relation):
        at = pl.ds(start, chunk)
        total = jnp.dot(
            x_own[at].reshape(chunk * block, width),
            w_all[mine, relation],
            preferred_element_type=jnp.float32,
        )
        for e in range(1, shards):
            peer = (mine + e) % shards
            total = total + jnp.dot(
                x_far[peer, at].reshape(chunk * block, width),
                w_all[peer, relation],
                preferred_element_type=jnp.float32,
            )
        return total.reshape(chunk, block, width)

    def transform(relation, carry):
        def part(i, inner):
            h_vmem[relation, pl.ds(i * chunk, chunk)] = full_dot(i * chunk, relation).astype(
                h_vmem.dtype
            )
            return inner

        return lax.fori_loop(0, blocks // chunk, part, carry)

    lax.fori_loop(0, relations, transform, 0)

    def own_part(i, carry):
        s_vmem[pl.ds(i * chunk, chunk)] = full_dot(i * chunk, relations)
        return carry

    lax.fori_loop(0, blocks // chunk, own_part, 0)
    for i in range(blocks):
        kinds = jnp.transpose(jnp.broadcast_to(type_ref[i : i + 1, :], (block, block)))
        kinds = jnp.concatenate([kinds] * (width // block), axis=1)
        total = s_vmem[i]
        for kind in range(bias_ref.shape[0]):
            total = total + jnp.where(kinds == kind, bias_ref[kind : kind + 1, :], 0.0)
        s_vmem[i] = total

    coef_copy.wait()
    stride = 4 if tiles % 4 == 0 else 1

    def multiply(i, carry):
        for j in range(stride):
            t = i * stride + j
            source = h_vmem[tile_relation[0, t], jnp.minimum(tile_source[0, t], blocks - 1)]
            products[t] = jnp.dot(coef[t], source, preferred_element_type=jnp.float32)
        return carry

    lax.fori_loop(0, tiles // stride, multiply, 0)
    slab = block // 4

    def accumulate(i, carry):
        target, at = i // 4, pl.ds((i % 4) * slab, slab)

        def step(k, total):
            for j in range(stride):
                t = k * stride + j
                counts = (tile_target[0, t] == target) & (tile_source[0, t] < blocks)
                total = total + products[t, at, :] * jnp.where(counts, 1.0, 0.0)
            return total

        s_vmem[target, at, :] = lax.fori_loop(0, tiles // stride, step, s_vmem[target, at, :])
        return carry

    lax.fori_loop(0, blocks * 4, accumulate, 0)
    s_copy = pltpu.make_async_copy(s_vmem, s_out, local_sem.at[5])

    def forward(step, e):
        other = partner(me, step, groups)
        return pltpu.make_async_remote_copy(
            src_ref=received.at[mine, other],
            dst_ref=received.at[mine, other],
            send_sem=pass_send.at[e - 1, step],
            recv_sem=pass_recv.at[e - 1, step],
            device_id=(me, (mine + e) % shards),
            device_id_type=MESH,
        )

    def arrived(step, carry):
        boundary(step).wait_recv()
        for e in range(1, shards):
            forward(step, e).start()
        return carry

    lax.fori_loop(1, groups - 1, arrived, 0)
    s_copy.start()
    arrived(groups - 1, 0)

    def finish(step, carry):
        boundary(step).wait_send()
        for e in range(1, shards):
            forward(step, e).wait_send()
            origin = (mine + shards - e) % shards
            other = partner(me, step, groups)
            pltpu.make_async_remote_copy(
                src_ref=received.at[origin, other],
                dst_ref=received.at[origin, other],
                send_sem=pass_send.at[e - 1, step],
                recv_sem=pass_recv.at[e - 1, step],
                device_id=(me, (mine + e) % shards),
                device_id_type=MESH,
            ).wait_recv()
        return carry

    lax.fori_loop(1, groups, finish, 0)
    w_copy.wait()
    s_copy.wait()


def tile_kernel(
    tile_source,
    tile_target,
    tile_relation,
    coef_hbm,
    s_hbm,
    received,
    w_hbm,
    out_hbm,
    coef,
    x_tiles,
    w_vmem,
    total,
    result,
    w_state,
    tile_sem,
    coef_sem,
    w_sem,
    base_sem,
):
    tiles = coef.shape[0]
    shards = w_vmem.shape[1]
    own = total.shape[0]

    total_copy = pltpu.make_async_copy(s_hbm, total, base_sem.at[0])

    def source_copy(t):
        return pltpu.make_async_copy(
            received.at[:, tile_source[0, t] - own], x_tiles.at[t], tile_sem.at[t]
        )

    def coef_copy(t):
        return pltpu.make_async_copy(coef_hbm.at[t], coef.at[t], coef_sem.at[t])

    def w_copy(r):
        return pltpu.make_async_copy(w_hbm.at[:, r], w_vmem.at[r], w_sem.at[r])

    for r in range(w_vmem.shape[0]):
        w_state[r] = 0

    def start(t, carry):
        relation = tile_relation[0, t]

        @pl.when(tile_source[0, t] >= own)
        def _():
            source_copy(t).start()

            @pl.when(w_state[relation] == 0)
            def _():
                w_copy(relation).start()
                w_state[relation] = 1

            coef_copy(t).start()

        return carry

    lax.fori_loop(0, tiles, start, 0)
    total_copy.start()
    total_copy.wait()

    def remote(t, carry):
        @pl.when(tile_source[0, t] >= own)
        def _():
            relation = tile_relation[0, t]

            @pl.when(w_state[relation] == 1)
            def _():
                w_copy(relation).wait()
                w_state[relation] = 2

            source_copy(t).wait()
            coef_copy(t).wait()
            moved = jnp.dot(x_tiles[t, 0], w_vmem[relation, 0], preferred_element_type=jnp.float32)
            for e in range(1, shards):
                moved = moved + jnp.dot(
                    x_tiles[t, e], w_vmem[relation, e], preferred_element_type=jnp.float32
                )
            total[tile_target[0, t]] += jnp.dot(
                coef[t], moved.astype(coef.dtype), preferred_element_type=jnp.float32
            )

        return carry

    lax.fori_loop(0, tiles, remote, 0)
    outs = []
    for i in range(own):
        result[i] = jnp.maximum(total[i], 0.0).astype(result.dtype)
        outs.append(pltpu.make_async_copy(result.at[i], out_hbm.at[i], base_sem.at[1 + i]))
        if i > 0:
            outs[i - 1].start()
    outs[-1].start()
    for copy in outs:
        copy.wait()


def per_device(
    groups,
    shards,
    features,
    rel_weight,
    self_weight,
    type_bias,
    node_type,
    tile_coef,
    tile_source,
    tile_target,
    tile_relation,
    send_block,
    send_live,
):
    rows, width = features.shape
    tiles, block, _ = tile_coef.shape
    relations = rel_weight.shape[0]
    kind = features.dtype
    smem = pl.BlockSpec(memory_space=pltpu.SMEM)
    vmem = pl.BlockSpec(memory_space=pltpu.VMEM)
    anywhere = pl.BlockSpec(memory_space=pl.ANY)
    dma = pltpu.SemaphoreType.DMA
    blocks = rows // block
    received, weights, base = pl.pallas_call(
        functools.partial(exchange_kernel, groups, shards, block),
        out_shape=(
            jax.ShapeDtypeStruct((shards, groups, block, width), kind),
            jax.ShapeDtypeStruct((shards, relations, width, width), kind),
            jax.ShapeDtypeStruct((blocks, block, width), jnp.float32),
        ),
        in_specs=[smem] * 5 + [vmem] * 2 + [anywhere] * 4,
        out_specs=(anywhere,) * 3,
        scratch_shapes=[
            pltpu.VMEM((groups, block, width), kind),
            pltpu.VMEM((blocks, block, width), kind),
            pltpu.VMEM((shards, blocks, block, width), kind),
            pltpu.VMEM((shards, relations + 1, width, width), kind),
            pltpu.VMEM((relations, blocks, block, width), kind),
            pltpu.VMEM((blocks, block, width), jnp.float32),
            pltpu.VMEM((tiles, block, block), kind),
            pltpu.VMEM((tiles, block, width), jnp.float32),
            dma((groups,)),
            dma((groups,)),
            dma((max(shards - 1, 1), groups)),
            dma((max(shards - 1, 1), groups)),
            dma((max(shards - 1, 1), 3)),
            dma((max(shards - 1, 1), 3)),
            dma((6,)),
        ],
        compiler_params=pltpu.CompilerParams(
            collective_id=0, has_side_effects=True, vmem_limit_bytes=VMEM
        ),
        name="exchange",
    )(
        send_block,
        send_live,
        tile_source,
        tile_target,
        tile_relation,
        type_bias,
        node_type.reshape(blocks, block),
        features.reshape(blocks, block, width),
        rel_weight,
        self_weight,
        tile_coef,
    )
    updated = pl.pallas_call(
        tile_kernel,
        out_shape=jax.ShapeDtypeStruct((blocks, block, width), kind),
        in_specs=[smem] * 3 + [anywhere] * 4,
        out_specs=anywhere,
        scratch_shapes=[
            pltpu.VMEM((tiles, block, block), kind),
            pltpu.VMEM((tiles, shards, block, width), kind),
            pltpu.VMEM((relations, shards, width, width), kind),
            pltpu.VMEM((blocks, block, width), jnp.float32),
            pltpu.VMEM((blocks, block, width), kind),
            pltpu.SMEM((relations,), jnp.int32),
            dma((tiles,)),
            dma((tiles,)),
            dma((relations,)),
            dma((1 + blocks,)),
        ],
        compiler_params=pltpu.CompilerParams(vmem_limit_bytes=VMEM),
        name="tiles",
    )(tile_source, tile_target, tile_relation, tile_coef, base, received, weights)
    return updated.reshape(rows, width)


def solution(mesh):
    placed = (
        P("graph", "feat"),
        P(None, "feat", None),
        P("feat", None),
        P(None, "feat"),
        P("graph"),
        P("graph", None, None),
        P("graph", None),
        P("graph", None),
        P("graph", None),
        P("graph", None),
        P("graph", None),
    )
    groups, shards = mesh.shape["graph"], mesh.shape["feat"]
    return jax.shard_map(
        functools.partial(per_device, groups, shards),
        mesh=mesh,
        in_specs=placed,
        out_specs=P("graph", "feat"),
        check_vma=False,
    )
```

```python
import functools

import jax
import jax.numpy as jnp
from jax import lax
from jax.experimental import pallas as pl
from jax.experimental.pallas import tpu as pltpu
from jax.sharding import PartitionSpec as P

MESH = pl.DeviceIdType.MESH
VMEM = 67_043_328


def partner(me, step, count):
    other, bit = 0, 1
    while bit < count:
        other = other + ((me // bit + step // bit) % 2) * bit
        bit *= 2
    return other


def exchange_kernel(
    groups,
    shards,
    block,
    send_block,
    send_live,
    tile_source,
    tile_target,
    tile_relation,
    bias_ref,
    type_ref,
    x_hbm,
    rel_ref,
    self_ref,
    coef_hbm,
    received,
    w_out,
    s_out,
    outgoing,
    x_own,
    x_far,
    w_all,
    h_vmem,
    s_vmem,
    coef,
    products,
    landed,
    send_sem,
    recv_sem,
    pass_send,
    pass_recv,
    side_send,
    side_recv,
    local_sem,
    keep_sem,
):
    me, mine = lax.axis_index("graph"), lax.axis_index("feat")
    blocks, _, width = x_own.shape
    relations = rel_ref.shape[0]
    tiles = coef.shape[0]

    def columns(shard):
        return pl.ds(pl.multiple_of(shard * width, width), width)

    barrier = pltpu.get_barrier_semaphore()

    def greet(step, carry):
        pl.semaphore_signal(
            barrier, inc=1, device_id=(partner(me, step, groups), mine), device_id_type=MESH
        )
        return carry

    lax.fori_loop(1, groups, greet, 0)
    for e in range(1, shards):
        pl.semaphore_signal(
            barrier, inc=1, device_id=(me, (mine + e) % shards), device_id_type=MESH
        )

    x_copy = pltpu.make_async_copy(x_hbm, x_own, local_sem.at[3])
    own_rel = pltpu.make_async_copy(
        rel_ref.at[:, :, columns(mine)], w_all.at[mine, pl.ds(0, relations)], local_sem.at[0]
    )
    own_self = pltpu.make_async_copy(
        self_ref.at[:, columns(mine)], w_all.at[mine, relations], local_sem.at[1]
    )
    coef_copy = pltpu.make_async_copy(coef_hbm, coef, local_sem.at[4])
    x_copy.start()
    own_rel.start()
    own_self.start()
    coef_copy.start()
    x_copy.wait()

    def gather(q, carry):
        picked = x_own[send_block[0, q]].astype(jnp.float32)
        outgoing[q] = (picked * send_live[0, q].astype(jnp.float32)).astype(outgoing.dtype)
        return carry

    lax.fori_loop(0, groups, gather, 0)
    pl.semaphore_wait(barrier, groups - 1 + shards - 1)

    def boundary(step):
        other = partner(me, step, groups)
        return pltpu.make_async_remote_copy(
            src_ref=outgoing.at[other],
            dst_ref=landed.at[me],
            send_sem=send_sem.at[step],
            recv_sem=recv_sem.at[step],
            device_id=(other, mine),
            device_id_type=MESH,
        )

    half = groups // 2
    inner = (me // half + me // max(half // 2, 1)) % 2

    def send(i, carry):
        boundary(1 + (i + inner * (half - 1)) % (groups - 1)).start()
        return carry

    lax.fori_loop(0, groups - 1, send, 0)

    def side(e):
        peer = (mine + e) % shards
        pairs = (
            (x_own, x_far.at[mine]),
            (self_ref.at[:, columns(peer)], w_all.at[mine, relations]),
            (rel_ref.at[:, :, columns(peer)], w_all.at[mine, pl.ds(0, relations)]),
        )
        return [
            pltpu.make_async_remote_copy(
                src_ref=src,
                dst_ref=dst,
                send_sem=side_send.at[e - 1, i],
                recv_sem=side_recv.at[e - 1, i],
                device_id=(me, peer),
                device_id_type=MESH,
            )
            for i, (src, dst) in enumerate(pairs)
        ]

    sides = [copy for e in range(1, shards) for copy in side(e)]
    for copy in sides:
        copy.start()
    own_rel.wait()
    own_self.wait()
    for copy in sides:
        copy.wait()
    w_copy = pltpu.make_async_copy(
        w_all.at[:, pl.ds(0, relations)], w_out, local_sem.at[2]
    )
    w_copy.start()

    chunk = 2

    def full_dot(start, relation):
        at = pl.ds(start, chunk)
        total = jnp.dot(
            x_own[at].reshape(chunk * block, width),
            w_all[mine, relation],
            preferred_element_type=jnp.float32,
        )
        for e in range(1, shards):
            peer = (mine + e) % shards
            total = total + jnp.dot(
                x_far[peer, at].reshape(chunk * block, width),
                w_all[peer, relation],
                preferred_element_type=jnp.float32,
            )
        return total.reshape(chunk, block, width)

    def transform(relation, carry):
        def part(i, inner):
            h_vmem[relation, pl.ds(i * chunk, chunk)] = full_dot(i * chunk, relation).astype(
                h_vmem.dtype
            )
            return inner

        return lax.fori_loop(0, blocks // chunk, part, carry)

    lax.fori_loop(0, relations, transform, 0)

    def own_part(i, carry):
        s_vmem[pl.ds(i * chunk, chunk)] = full_dot(i * chunk, relations)
        return carry

    lax.fori_loop(0, blocks // chunk, own_part, 0)
    for i in range(blocks):
        kinds = jnp.transpose(jnp.broadcast_to(type_ref[i : i + 1, :], (block, block)))
        kinds = jnp.concatenate([kinds] * (width // block), axis=1)
        total = s_vmem[i]
        for kind in range(bias_ref.shape[0]):
            total = total + jnp.where(kinds == kind, bias_ref[kind : kind + 1, :], 0.0)
        s_vmem[i] = total

    coef_copy.wait()
    stride = 4 if tiles % 4 == 0 else 1

    def multiply(i, carry):
        for j in range(stride):
            t = i * stride + j
            source = h_vmem[tile_relation[0, t], jnp.minimum(tile_source[0, t], blocks - 1)]
            products[t] = jnp.dot(coef[t], source, preferred_element_type=jnp.float32)
        return carry

    lax.fori_loop(0, tiles // stride, multiply, 0)
    slab = block // 4

    def accumulate(i, carry):
        target, at = i // 4, pl.ds((i % 4) * slab, slab)

        def step(k, total):
            for j in range(stride):
                t = k * stride + j
                counts = (tile_target[0, t] == target) & (tile_source[0, t] < blocks)
                total = total + products[t, at, :] * jnp.where(counts, 1.0, 0.0)
            return total

        s_vmem[target, at, :] = lax.fori_loop(0, tiles // stride, step, s_vmem[target, at, :])
        return carry

    lax.fori_loop(0, blocks * 4, accumulate, 0)
    s_copy = pltpu.make_async_copy(s_vmem, s_out, local_sem.at[5])

    def forward(step, e):
        other = partner(me, step, groups)
        return pltpu.make_async_remote_copy(
            src_ref=landed.at[other],
            dst_ref=received.at[mine, other],
            send_sem=pass_send.at[e - 1, step],
            recv_sem=pass_recv.at[e - 1, step],
            device_id=(me, (mine + e) % shards),
            device_id_type=MESH,
        )

    def keep(step):
        other = partner(me, step, groups)
        return pltpu.make_async_copy(
            landed.at[other], received.at[mine, other], keep_sem.at[step]
        )

    quarter = max(groups // 4, 1)

    def arrived(i, carry):
        turn = i // quarter
        step = ((turn % 2) * 2 + (turn // 2 + inner) % 2) * quarter + i % quarter

        @pl.when(step > 0)
        def _():
            boundary(step).wait_recv()
            keep(step).start()
            for e in range(1, shards):
                forward(step, e).start()

        return carry

    lax.fori_loop(0, groups - 1, arrived, 0)
    s_copy.start()
    lax.fori_loop(groups - 1, groups, arrived, 0)

    def finish(step, carry):
        boundary(step).wait_send()
        keep(step).wait()
        for e in range(1, shards):
            forward(step, e).wait_send()
            origin = (mine + shards - e) % shards
            other = partner(me, step, groups)
            pltpu.make_async_remote_copy(
                src_ref=received.at[origin, other],
                dst_ref=received.at[origin, other],
                send_sem=pass_send.at[e - 1, step],
                recv_sem=pass_recv.at[e - 1, step],
                device_id=(me, (mine + e) % shards),
                device_id_type=MESH,
            ).wait_recv()
        return carry

    lax.fori_loop(1, groups, finish, 0)
    w_copy.wait()
    s_copy.wait()


def tile_kernel(
    tile_source,
    tile_target,
    tile_relation,
    coef_hbm,
    s_hbm,
    received,
    w_hbm,
    out_hbm,
    coef,
    x_tiles,
    w_vmem,
    total,
    result,
    w_state,
    chosen,
    tile_sem,
    coef_sem,
    w_sem,
    base_sem,
):
    tiles = coef.shape[0]
    shards = w_vmem.shape[1]
    own = result.shape[0]

    total_copy = pltpu.make_async_copy(s_hbm, total.at[pl.ds(0, own)], base_sem.at[0])
    total_copy.start()

    def source_copy(j, t):
        return pltpu.make_async_copy(
            received.at[:, tile_source[0, t] - own], x_tiles.at[j], tile_sem.at[j]
        )

    def coef_copy(j, t):
        return pltpu.make_async_copy(coef_hbm.at[t], coef.at[j], coef_sem.at[j])

    def w_copy(r):
        return pltpu.make_async_copy(w_hbm.at[:, r], w_vmem.at[r], w_sem.at[r])

    for r in range(w_vmem.shape[0]):
        w_state[r] = 0

    def start(t, count):
        relation = tile_relation[0, t]
        is_remote = tile_source[0, t] >= own

        @pl.when(is_remote)
        def _():
            chosen[count] = t
            source_copy(count, t).start()

            @pl.when(w_state[relation] == 0)
            def _():
                w_copy(relation).start()
                w_state[relation] = 1

            coef_copy(count, t).start()

        return count + is_remote.astype(jnp.int32)

    count = lax.fori_loop(0, tiles, start, 0)
    total_copy.wait()

    def ready(j):
        t = chosen[j]
        relation = tile_relation[0, t]

        @pl.when(w_state[relation] == 1)
        def _():
            w_copy(relation).wait()
            w_state[relation] = 2

        source_copy(j, t).wait()
        coef_copy(j, t).wait()

    def moved(j, relation):
        value = jnp.dot(x_tiles[j, 0], w_vmem[relation, 0], preferred_element_type=jnp.float32)
        for e in range(1, shards):
            value = value + jnp.dot(
                x_tiles[j, e], w_vmem[relation, e], preferred_element_type=jnp.float32
            )
        value = value.astype(coef.dtype)
        return jnp.dot(coef[j], value, preferred_element_type=jnp.float32)

    def pair(i, carry):
        first, second = 2 * i, 2 * i + 1
        both = second < count
        ready(first)

        @pl.when(both)
        def _():
            ready(second)

        second = jnp.where(both, second, first)
        t, u = chosen[first], chosen[second]
        one = moved(first, tile_relation[0, t])
        two = moved(second, tile_relation[0, u])
        total[tile_target[0, t]] += one
        total[jnp.where(both, tile_target[0, u], own)] += two
        return carry

    lax.fori_loop(0, (count + 1) // 2, pair, 0)
    outs = []
    for i in range(own):
        result[i] = jnp.maximum(total[i], 0.0).astype(result.dtype)
        outs.append(pltpu.make_async_copy(result.at[i], out_hbm.at[i], base_sem.at[1 + i]))
        if i > 0:
            outs[i - 1].start()
    outs[-1].start()
    for copy in outs:
        copy.wait()


def per_device(
    groups,
    shards,
    features,
    rel_weight,
    self_weight,
    type_bias,
    node_type,
    tile_coef,
    tile_source,
    tile_target,
    tile_relation,
    send_block,
    send_live,
):
    rows, width = features.shape
    tiles, block, _ = tile_coef.shape
    relations = rel_weight.shape[0]
    kind = features.dtype
    smem = pl.BlockSpec(memory_space=pltpu.SMEM)
    vmem = pl.BlockSpec(memory_space=pltpu.VMEM)
    anywhere = pl.BlockSpec(memory_space=pl.ANY)
    dma = pltpu.SemaphoreType.DMA
    blocks = rows // block
    received, weights, base = pl.pallas_call(
        functools.partial(exchange_kernel, groups, shards, block),
        out_shape=(
            jax.ShapeDtypeStruct((shards, groups, block, width), kind),
            jax.ShapeDtypeStruct((shards, relations, width, width), kind),
            jax.ShapeDtypeStruct((blocks, block, width), jnp.float32),
        ),
        in_specs=[smem] * 5 + [vmem] * 2 + [anywhere] * 4,
        out_specs=(anywhere,) * 3,
        scratch_shapes=[
            pltpu.VMEM((groups, block, width), kind),
            pltpu.VMEM((blocks, block, width), kind),
            pltpu.VMEM((shards, blocks, block, width), kind),
            pltpu.VMEM((shards, relations + 1, width, width), kind),
            pltpu.VMEM((relations, blocks, block, width), kind),
            pltpu.VMEM((blocks, block, width), jnp.float32),
            pltpu.VMEM((tiles, block, block), kind),
            pltpu.VMEM((tiles, block, width), jnp.float32),
            pltpu.VMEM((groups, block, width), kind),
            dma((groups,)),
            dma((groups,)),
            dma((max(shards - 1, 1), groups)),
            dma((max(shards - 1, 1), groups)),
            dma((max(shards - 1, 1), 3)),
            dma((max(shards - 1, 1), 3)),
            dma((6,)),
            dma((groups,)),
        ],
        compiler_params=pltpu.CompilerParams(
            collective_id=0, has_side_effects=True, vmem_limit_bytes=VMEM
        ),
        name="exchange",
    )(
        send_block,
        send_live,
        tile_source,
        tile_target,
        tile_relation,
        type_bias,
        node_type.reshape(blocks, block),
        features.reshape(blocks, block, width),
        rel_weight,
        self_weight,
        tile_coef,
    )
    updated = pl.pallas_call(
        tile_kernel,
        out_shape=jax.ShapeDtypeStruct((blocks, block, width), kind),
        in_specs=[smem] * 3 + [anywhere] * 4,
        out_specs=anywhere,
        scratch_shapes=[
            pltpu.VMEM((tiles, block, block), kind),
            pltpu.VMEM((tiles, shards, block, width), kind),
            pltpu.VMEM((relations, shards, width, width), kind),
            pltpu.VMEM((blocks + 1, block, width), jnp.float32),
            pltpu.VMEM((blocks, block, width), kind),
            pltpu.SMEM((relations,), jnp.int32),
            pltpu.SMEM((tiles,), jnp.int32),
            dma((tiles,)),
            dma((tiles,)),
            dma((relations,)),
            dma((1 + blocks,)),
        ],
        compiler_params=pltpu.CompilerParams(vmem_limit_bytes=VMEM),
        name="tiles",
    )(tile_source, tile_target, tile_relation, tile_coef, base, received, weights)
    return updated.reshape(rows, width)


def solution(mesh):
    placed = (
        P("graph", "feat"),
        P(None, "feat", None),
        P("feat", None),
        P(None, "feat"),
        P("graph"),
        P("graph", None, None),
        P("graph", None),
        P("graph", None),
        P("graph", None),
        P("graph", None),
        P("graph", None),
    )
    groups, shards = mesh.shape["graph"], mesh.shape["feat"]
    return jax.shard_map(
        functools.partial(per_device, groups, shards),
        mesh=mesh,
        in_specs=placed,
        out_specs=P("graph", "feat"),
        check_vma=False,
    )
```
